32 devices in a mesh: dp: 8 (over z, y), group: 4 (over x, core).
Axes of the slice: x: 2, y: 2, z: 4, core: 2. Of those that a mesh axis runs over, the one named last changes fastest.
Arguments:
- features: bfloat16 [4096, 512], P(('dp', 'group')), may hold values from -6 to 6
- head_weight: bfloat16 [512, 512], replicated, may hold values from -0.25 to 0.25
- owner_of_image: int32 [4096, 1], P(('dp', 'group')), may hold values from 0 to 7; in each aligned block of 128 rows (0 to 127, 128 to 255, ...) at most 32 rows name the same one
- class_slot: int32 [4096], P(('dp', 'group')), may hold values from 0 to 49
- is_query: int32 [4096], P(('dp', 'group')), may hold values 0 or 1
- episode_ways: int32 [32], P(('dp', 'group')), may hold values from 5 to 50
Outputs:
- grad_features: bfloat16 [4096, 512], P(('dp', 'group'))
- grad_weight: float32 [512, 512], replicated
- losses: float32 [32], P(('dp', 'group'))
The draws below stay inside these ranges and needn't reach their ends.
Inputs may be any that keep to these rules, and one draw needn't show every extreme that they name: `owner_of_image`: among the rows of one device at most 32 name any one owner, a bound that some block reaches.
All inputs are finite; a program needn't handle non-finite values. No bound on the sum of `is_query` on one device may be relied on, other than what follows from the above.
Results may differ from the reference program's by a relative error of at most 0.0037.
The reference program's roundings to bfloat16 on the way count: a program that leaves them out, or rounds other values in their place, can miss the bound.
Values may be sent and summed in bfloat16 or wider, within the bound.
No kernel may reach another device: no remote copies, remote signals or barrier semaphores. Data moves between devices by JAX's collectives and lax.ppermute only.
A program may use at most 64 MiB of HBM per device.

```python
import math
import jax
import jax.numpy as jnp
import numpy as np
from jax import lax

D = 512
WAYS_MAX = 50
ROWS_DEV = 128
EP_DEV = 1
CAP = 32
IMAGES = 4096
EPISODES = 32
N_DP = 8
N_GROUP = 4


def touch_ends(array, rng, least, top_value):
    longest = array.shape.index(max(array.shape))
    spots = []
    for shift in (0, 1):
        where = [jax.random.randint(jax.random.fold_in(rng, axis), (), 0, length) for axis, length in enumerate(array.shape)]
        where[longest] = (where[longest] + shift) % array.shape[longest]
        spots.append(tuple(where))
    return array.at[spots[0]].set(least).at[spots[1]].set(top_value)


def block_levels(stream_key, extent, split, least, high):
    level, own = 1.0, jax.random.fold_in(stream_key, 6)
    for axis_at, shards_of in split:
        draws = jnp.exp(jax.random.uniform(jax.random.fold_in(own, axis_at), (shards_of,), jnp.float32, least / len(split), high / len(split)))
        level = level * jnp.repeat(draws, extent[axis_at] // shards_of).reshape([-1 if axis == axis_at else 1 for axis in range(len(extent))])
    return level


def routed_block(stream_key, own, number, rows, number_of, top, bound, skew):
    ranking = jax.random.permutation(stream_key, number_of)
    packed, common = portions_of(number_of, rows * top, bound, skew, True), portions_of(number_of, rows * top, bound, skew, False)
    places = jnp.arange(number_of)

    def named(sizes, rotation):
        used = int((sizes > 0).sum())
        fixed = max(1, used // 4)
        moved = fixed + (places - fixed + rotation * (used - fixed)) % max(1, number_of - fixed)
        return jnp.zeros((number_of,), jnp.int32).at[ranking[jnp.where(places < fixed, places, moved)]].set(jnp.asarray(sizes, jnp.int32))

    sizes = jnp.where(number % 4 == 0, named(packed, number // 4), named(common, number - number // 4 - 1))
    mixed = jax.random.permutation(jax.random.fold_in(own, 3), number_of)
    source_of, taker = mixed[0:number_of // 2 * 2:2], mixed[1:number_of // 2 * 2:2]
    room = jnp.minimum(sizes[source_of] - 1, bound - sizes[taker]) // 2
    room = jnp.where((source_of == ranking[0]) | (taker == ranking[0]) | (sizes[taker] == 0), 0, jnp.maximum(room, 0))
    moved = jax.random.randint(jax.random.fold_in(own, 4), (number_of // 2,), 0, 1 << 20) % (room + 1)
    sizes = sizes.at[source_of].add(-moved).at[taker].add(moved)
    labels = jnp.searchsorted(jnp.cumsum(sizes), jnp.arange(rows * top), side="right").astype(jnp.int32)
    grid = labels.reshape(top, rows).T
    grid = grid[jax.random.permutation(jax.random.fold_in(own, 1), rows)]
    rotation = jax.random.randint(jax.random.fold_in(own, 2), (rows, 1), 0, top)
    return jnp.take_along_axis(grid, (jnp.arange(top)[None, :] + rotation) % top, axis=1)


def portions_of(number_of, total, most, lean, full):
    weights = [(1 << 20) // math.isqrt(grade ** lean) + 1 for grade in range(1, number_of + 1)]
    largest = most if full else min(most, max(-(-total // number_of), total * weights[0] // sum(weights)))
    least = 1 if total - largest >= number_of - 1 else 0
    given, rest = [largest] + [least] * (number_of - 1), total - largest - least * (number_of - 1)
    while rest > 0:
        free = [i for i in range(1, number_of) if given[i] < largest] or [i for i in range(1, number_of) if given[i] < most]
        mass, budget = sum([weights[i] for i in free]), rest
        for i in free:
            addition = min(most - given[i], max(1, budget * weights[i] // mass), rest)
            given[i] = given[i] + addition
            rest = rest - addition
    return np.array(given)


def normal_values(stream_key, shape, deviation, bound, shards=(), kind=jnp.bfloat16):
    values = deviation * jax.random.normal(stream_key, shape, jnp.float32)
    if shards:
        values = values * block_levels(stream_key, shape, shards, -0.22, 0.18)
    return jnp.clip(values, -bound, bound).astype(kind)


def setup_inputs(seed: int = 0) -> dict:
    arg_keys = jax.random.split(jax.random.key(seed), 7)
    features = normal_values(arg_keys[0], (IMAGES, D), 1.0, 6.0, ((0, 32),))
    head_weight = normal_values(arg_keys[1], (D, D), D ** -0.5, 0.25)
    owner_of_image_keys = jax.random.split(jax.random.fold_in(arg_keys[2], 1), IMAGES // ROWS_DEV)
    owner_of_image_turns = jax.random.permutation(jax.random.fold_in(arg_keys[2], 3), IMAGES // ROWS_DEV)
    owner_of_image = jax.vmap(lambda own, number: routed_block(jax.random.fold_in(arg_keys[2], 2), own, number, ROWS_DEV, N_DP, 1, CAP, 2))(owner_of_image_keys, owner_of_image_turns).reshape((IMAGES, 1))
    class_slot = touch_ends(jax.random.randint(arg_keys[3], (IMAGES,), 0, EP_DEV * WAYS_MAX), jax.random.fold_in(arg_keys[3], 1), 0, (EP_DEV * WAYS_MAX) - 1).astype(jnp.int32)
    is_query = touch_ends((jax.random.randint(arg_keys[4], (IMAGES,), 0, 2) < 1).astype(jnp.int32), jax.random.fold_in(arg_keys[4], 1), 0, 1)
    episode_ways = touch_ends(jax.random.randint(arg_keys[5], (EPISODES,), 5, WAYS_MAX + 1), jax.random.fold_in(arg_keys[5], 1), 5, WAYS_MAX).astype(jnp.int32)
    return dict(features=features, head_weight=head_weight, owner_of_image=owner_of_image, class_slot=class_slot, is_query=is_query, episode_ways=episode_ways)


def episode_losses(embeds, codes, ways_table):
    count_ep = ways_table.shape[0]
    is_live = codes > 0
    code_value = jnp.maximum(codes - 1, 0)
    query_rows = is_live & (code_value % 2 == 1)
    support_rows = is_live & (code_value % 2 == 0)
    slot_value = code_value // 2
    episode = slot_value // WAYS_MAX
    raw_class = slot_value % WAYS_MAX
    episode_hot = episode[:, None] == jnp.arange(count_ep, dtype=jnp.int32)[None, :]
    row_ways = lax.optimization_barrier(jnp.sum(jnp.where(episode_hot, ways_table[None, :], 0), axis=1))
    label_id = episode * WAYS_MAX + raw_class % row_ways
    classes = jnp.arange(count_ep * WAYS_MAX, dtype=jnp.int32)
    class_hot = label_id[:, None] == classes[None, :]
    support_hot = (class_hot & support_rows[:, None]).astype(jnp.float32)
    counts = lax.optimization_barrier(jnp.sum(support_hot, axis=0))
    class_sums = jnp.dot(support_hot.T, embeds, precision=lax.Precision.HIGHEST)
    prototypes = class_sums / jnp.maximum(counts, 1.0)[:, None]
    class_ways = jnp.repeat(ways_table, WAYS_MAX)
    class_valid = classes % WAYS_MAX < class_ways
    allowed = (episode[:, None] == (classes // WAYS_MAX)[None, :]) & class_valid[None, :]
    cross_term = jnp.dot(embeds, prototypes.T, precision=lax.Precision.HIGHEST)
    distance = lax.optimization_barrier(jnp.sum(embeds * embeds, axis=1))[:, None] - 2.0 * cross_term + lax.optimization_barrier(jnp.sum(prototypes * prototypes, axis=1))[None, :]
    scores = -distance * D ** (-0.5)
    masked = jnp.where(allowed, scores, -1e+30)
    row_max = lax.optimization_barrier(jnp.max(masked, axis=1, keepdims=True))
    log_total = row_max[:, 0] + jnp.log(lax.optimization_barrier(jnp.sum(jnp.exp(masked - row_max), axis=1)))
    picked = lax.optimization_barrier(jnp.sum(jnp.where(class_hot, scores, 0.0), axis=1))
    per_query = jnp.where(query_rows, log_total - picked, 0.0)
    hot_float = episode_hot.astype(jnp.float32)
    query_count = lax.optimization_barrier(jnp.sum(hot_float * query_rows[:, None].astype(jnp.float32), axis=0))
    return lax.optimization_barrier(jnp.sum(hot_float * per_query[:, None], axis=0)) / jnp.maximum(query_count, 1.0)

def reference(features, head_weight, owner_of_image, class_slot, is_query, episode_ways):
    devices = N_DP * N_GROUP
    capacity = 2 * ROWS_DEV // N_DP
    slot_count = N_DP * capacity
    embeds = jnp.dot(features, head_weight, preferred_element_type=jnp.float32).astype(jnp.bfloat16)
    target = owner_of_image[:, 0].reshape(devices, ROWS_DEV)
    one_hot = (target[:, :, None] == jnp.arange(N_DP, dtype=jnp.int32)[None, None, :]).astype(jnp.int32)
    before = jnp.cumsum(one_hot, axis=1) - one_hot
    position = lax.optimization_barrier(jnp.sum(one_hot * before, axis=2))
    device_ids = jnp.arange(devices, dtype=jnp.int32)
    source = device_ids // N_GROUP
    group_id = device_ids % N_GROUP
    owner = target * N_GROUP + group_id[:, None]
    place = (owner * slot_count + source[:, None] * capacity + position).reshape(-1)
    codes = class_slot * 2 + is_query + 1
    table = jnp.zeros((devices * slot_count,), jnp.int32).at[place].set(jnp.arange(IMAGES, dtype=jnp.int32) + 1)
    table = table.reshape(devices, slot_count)

    def per_owner(inputs):
        index_row, ways_row = inputs
        is_live = index_row > 0
        pick_row = jnp.maximum(index_row - 1, 0)
        rows = jnp.where(is_live[:, None], embeds[pick_row].astype(jnp.float32), 0.0)
        code_row = jnp.where(is_live, codes[pick_row], 0)
        values, pull = jax.vjp(lambda e: episode_losses(e, code_row, ways_row), rows)
        grads = pull(jnp.ones_like(values))[0].astype(jnp.bfloat16)
        return (grads, values)
    grads, losses = lax.map(per_owner, (table, episode_ways.reshape(devices, EP_DEV)))
    grad_rows = grads.reshape(-1, D)[place]
    grad_features = lax.dot_general(grad_rows, head_weight, (((1,), (1,)), ((), ())), preferred_element_type=jnp.float32).astype(jnp.bfloat16)
    grad_weight = lax.dot_general(features, grad_rows, (((0,), (0,)), ((), ())), preferred_element_type=jnp.float32)
    return (grad_features, grad_weight, losses.reshape(-1))
```

```python
import functools

import jax
import jax.numpy as jnp
from jax import lax
from jax.experimental import pallas as pl
from jax.experimental.pallas import tpu as pltpu
from jax.sharding import PartitionSpec as P

D = 512
WAYS_MAX = 50
CODE_ROWS = 8


def episode_losses(embeds, codes, ways_table):
    count_ep = ways_table.shape[0]
    is_live = codes > 0
    code_value = jnp.maximum(codes - 1, 0)
    query_rows = is_live & (code_value % 2 == 1)
    support_rows = is_live & (code_value % 2 == 0)
    slot_value = code_value // 2
    episode = slot_value // WAYS_MAX
    raw_class = slot_value % WAYS_MAX
    episode_hot = episode[:, None] == jnp.arange(count_ep, dtype=jnp.int32)[None, :]
    row_ways = jnp.sum(jnp.where(episode_hot, ways_table[None, :], 0), axis=1)
    label_id = episode * WAYS_MAX + raw_class % row_ways
    classes = jnp.arange(count_ep * WAYS_MAX, dtype=jnp.int32)
    class_hot = label_id[:, None] == classes[None, :]
    support_hot = (class_hot & support_rows[:, None]).astype(jnp.float32)
    counts = jnp.sum(support_hot, axis=0)
    class_sums = jnp.dot(support_hot.T, embeds, precision=lax.Precision.HIGHEST)
    prototypes = class_sums / jnp.maximum(counts, 1.0)[:, None]
    class_ways = jnp.repeat(ways_table, WAYS_MAX)
    class_valid = classes % WAYS_MAX < class_ways
    allowed = (episode[:, None] == (classes // WAYS_MAX)[None, :]) & class_valid[None, :]
    cross_term = jnp.dot(embeds, prototypes.T, precision=lax.Precision.HIGHEST)
    distance = (
        jnp.sum(embeds * embeds, axis=1)[:, None]
        - 2.0 * cross_term
        + jnp.sum(prototypes * prototypes, axis=1)[None, :]
    )
    scores = -distance * D ** (-0.5)
    masked = jnp.where(allowed, scores, -1e30)
    row_max = jnp.max(masked, axis=1, keepdims=True)
    log_total = row_max[:, 0] + jnp.log(jnp.sum(jnp.exp(masked - row_max), axis=1))
    picked = jnp.sum(jnp.where(class_hot, scores, 0.0), axis=1)
    per_query = jnp.where(query_rows, log_total - picked, 0.0)
    hot_float = episode_hot.astype(jnp.float32)
    query_count = jnp.sum(hot_float * query_rows[:, None].astype(jnp.float32), axis=0)
    return jnp.sum(hot_float * per_query[:, None], axis=0) / jnp.maximum(query_count, 1.0)


def times_transpose(left, right):
    return lax.dot_general(
        left, right, (((1,), (1,)), ((), ())), preferred_element_type=jnp.float32
    )


def inner_rows(left, right):
    return lax.dot_general(
        left, right, (((0,), (0,)), ((), ())), preferred_element_type=jnp.float32
    )


def routed(features, head_weight, owner_of_image, class_slot, is_query, episode_ways):
    peers = lax.axis_size("dp")
    row_count = features.shape[0]
    capacity = 2 * row_count // peers
    target = owner_of_image[:, 0]
    one_hot = (target[:, None] == jnp.arange(peers, dtype=jnp.int32)[None, :]).astype(jnp.int32)
    before = jnp.cumsum(one_hot, axis=0) - one_hot
    position = jnp.sum(one_hot * before, axis=1)
    flat_slot = target * capacity + position
    codes = class_slot * 2 + is_query + 1
    send_rows = (
        jnp.zeros((peers * capacity, D), jnp.bfloat16)
        .at[flat_slot]
        .set(features)
        .reshape(peers, capacity, D)
    )
    send_codes = (
        jnp.zeros((peers * capacity,), jnp.int32).at[flat_slot].set(codes).reshape(peers, capacity)
    )
    got_rows, got_codes = (
        lax.all_to_all(send_rows, "dp", split_axis=0, concat_axis=0, tiled=True),
        lax.all_to_all(send_codes, "dp", split_axis=0, concat_axis=0, tiled=True),
    )
    got_rows = got_rows.reshape(peers * capacity, D)
    got_codes = got_codes.reshape(peers * capacity)
    got_embeds = jnp.dot(got_rows, head_weight, preferred_element_type=jnp.float32).astype(
        jnp.bfloat16
    )
    losses, pull = jax.vjp(
        lambda e: episode_losses(e, got_codes, episode_ways), got_embeds.astype(jnp.float32)
    )
    grad_embeds = pull(jnp.ones_like(losses))[0].astype(jnp.bfloat16)
    partial_value = inner_rows(got_rows, grad_embeds)
    outgoing = times_transpose(grad_embeds, head_weight).astype(jnp.bfloat16)
    returned = lax.all_to_all(
        outgoing.reshape(peers, capacity, D), "dp", split_axis=0, concat_axis=0, tiled=True
    )
    own_rows = returned.reshape(peers * capacity, D)[flat_slot]
    grad_weight = lax.psum(partial_value, ("dp", "group"))
    return (own_rows, grad_weight, losses)


def pack_kernel(features, owner, slot, query, ways, block):
    rows = features.shape[0]
    block[:rows, :] = features[...]
    line = lax.broadcasted_iota(jnp.int32, (CODE_ROWS, rows), 0)
    way = jnp.full((1, rows), ways[0], jnp.int32)
    fields = jnp.where(
        line == 0,
        owner[...],
        jnp.where(line == 1, slot[...], jnp.where(line == 2, query[...], way)),
    )
    block[rows:, :] = jnp.zeros((CODE_ROWS, D), jnp.bfloat16)
    block[rows:, :rows] = fields.astype(jnp.float32).astype(jnp.bfloat16)


def embed_kernel(block, weight, embeds, turned, codes):
    rows = embeds.shape[0]
    rows_in = block[:rows, :]
    values = jnp.dot(rows_in, weight[...], preferred_element_type=jnp.float32).astype(jnp.bfloat16)
    embeds[...] = values
    turned[...] = rows_in.T
    wide = values.astype(jnp.float32)
    squares = jnp.sum(wide * wide, axis=1, keepdims=True)
    line = lax.broadcasted_iota(jnp.int32, (CODE_ROWS, rows), 0)
    lengths = jnp.broadcast_to(squares, (rows, 128)).T[:CODE_ROWS, :]
    codes[...] = jnp.where(
        line == 4, lengths, block[rows:, :rows].astype(jnp.float32)
    )


def split(value):
    high = value.astype(jnp.bfloat16)
    return high, (value - high.astype(jnp.float32)).astype(jnp.bfloat16)


def dot(left, right, on=(1, 0)):
    return lax.dot_general(
        left, right, (((on[0],), (on[1],)), ((), ())), preferred_element_type=jnp.float32
    )


def main_kernel(count, place, *refs):
    embeds_in, turned_in, codes_in = refs[:count], refs[count : 2 * count], refs[2 * count : 3 * count]
    weight = refs[3 * count]
    grad_rows, keep, give, loss = refs[3 * count + 1 : 3 * count + 5]
    embeds, turned, codes, grads, cross, hot_s, g_high, g_low = refs[3 * count + 5 :]
    rows = embeds_in[0].shape[0]
    total = rows * count
    classes = count * WAYS_MAX
    scale = D ** (-0.5)

    for k in range(count):
        start = pl.multiple_of(place[k] * rows, rows)
        embeds[pl.ds(start, rows), :] = embeds_in[k][...]
        turned[:, pl.ds(start, rows)] = turned_in[k][...]
        codes[pl.ds(place[k], 1)] = codes_in[k][...][None]

    def field(line):
        return jnp.concatenate([codes[p, line : line + 1, :] for p in range(count)], axis=1)

    owner, slot, query, length = field(0), field(1), field(2), field(4)
    ways = jnp.zeros_like(owner)
    queries = jnp.zeros_like(owner)
    for p in range(count):
        mine = owner == float(p)
        ways = jnp.where(mine, codes[p, 3:4, 0:1], ways)
        total_q = jnp.sum(jnp.where(mine, query, 0.0), axis=1, keepdims=True)
        queries = jnp.where(mine, total_q, queries)
    share = query / jnp.maximum(queries, 1.0)
    label = slot - jnp.floor((slot + 0.5) / ways) * ways
    first = (owner * float(WAYS_MAX)).astype(jnp.int32)
    last = first + ways.astype(jnp.int32)
    own_class = first + label.astype(jnp.int32)
    support_class = jnp.where(query > 0.5, -1, own_class)

    ids = lax.broadcasted_iota(jnp.int32, (classes, total), 0)
    hot_value = jnp.where(ids == support_class, 1.0, 0.0)
    counts = jnp.sum(hot_value, axis=1, keepdims=True)
    hot_s[...] = hot_value.astype(jnp.bfloat16)
    per_class = 1.0 / jnp.maximum(counts, 1.0)
    protos = dot(hot_s[...], embeds[...]) / jnp.maximum(counts, 1.0)
    p_high, p_low = split(protos)
    p_length = jnp.sum(protos * protos, axis=1, keepdims=True)

    g_sum = jnp.zeros((classes, 1), jnp.float32)
    loss_sum = jnp.zeros((1, 1), jnp.float32)
    row_sums = []
    step = min(total, 256)
    for at in range(0, total, step):
        part = slice(at, at + step)
        e = embeds[part, :]
        product = dot(p_high, e, (1, 1)) + dot(p_low, e, (1, 1))
        scores = -(length[:, part] - 2.0 * product + p_length) * scale
        c = lax.broadcasted_iota(jnp.int32, (classes, step), 0)
        masked = jnp.where((c >= first[:, part]) & (c < last[:, part]), scores, -1e30)
        top = jnp.max(masked, axis=0, keepdims=True)
        powers = jnp.exp(masked - top)
        norm = jnp.sum(powers, axis=0, keepdims=True)
        is_own = c == own_class[:, part]
        picked = jnp.sum(jnp.where(is_own, scores, 0.0), axis=0, keepdims=True)
        mine = owner[:, part] == place[0].astype(jnp.float32)
        losses = share[:, part] * (top + jnp.log(norm) - picked)
        loss_sum += jnp.sum(jnp.where(mine, losses, 0.0), axis=1, keepdims=True)
        g = (powers * (1.0 / norm) - jnp.where(is_own, 1.0, 0.0)) * (
            share[:, part] * (2.0 * scale)
        )
        g_sum += jnp.sum(g, axis=1, keepdims=True)
        row_sums.append(jnp.sum(g, axis=0, keepdims=True))
        high, low = split(g)
        g_high[:, part] = high
        g_low[:, part] = low
    loss[...] = loss_sum

    e = embeds[...]
    d_protos = dot(g_high[...], e) + dot(g_low[...], e) - g_sum * protos
    s_high, s_low = split(d_protos * per_class)
    for at in range(0, total, step):
        part = slice(at, at + step)
        value = (
            dot(g_high[:, part], p_high, (0, 0))
            + dot(g_low[:, part], p_high, (0, 0))
            + dot(g_high[:, part], p_low, (0, 0))
            + dot(hot_s[:, part], s_high, (0, 0))
            + dot(hot_s[:, part], s_low, (0, 0))
        )
        back = jnp.broadcast_to(row_sums[at // step], (128, step)).T[:, :1]
        value = value - back * embeds[part, :].astype(jnp.float32)
        grads[part, :] = value.astype(jnp.bfloat16)

    half = D // 2
    bit = place[count]
    keep_at = pl.multiple_of(bit * half, half)
    give_at = pl.multiple_of((1 - bit) * half, half)
    give[...] = dot(turned[pl.ds(give_at, half), :], grads[...])
    keep[...] = dot(turned[pl.ds(keep_at, half), :], grads[...])
    own = grads[pl.ds(pl.multiple_of(place[0] * rows, rows), rows), :]
    grad_rows[...] = dot(own, weight[...], (1, 1)).astype(jnp.bfloat16)


def vmem(n):
    return [pl.BlockSpec(memory_space=pltpu.VMEM)] * n


def gathered(features, head_weight, owner_of_image, class_slot, is_query, episode_ways):
    count = lax.axis_size("dp")
    groups = lax.axis_size("group")
    rows = features.shape[0]
    classes = count * WAYS_MAX
    total = rows * count

    order = [d for d in range(0, count, 2)] + [d for d in range(count - 1, 0, -1) if d % 2]
    ahead = [(order[i], order[(i + 1) % count]) for i in range(count)]
    behind = [(b, a) for a, b in ahead]
    spot = jnp.array([order.index(d) for d in range(count)], jnp.int32)[lax.axis_index("dp")]
    steps = [0]
    for k in range(1, count // 2 + 1):
        steps.append(-k)
        if k <= (count - 1) // 2:
            steps.append(k)
    place = jnp.array(order, jnp.int32)[(spot + jnp.array(steps, jnp.int32)) % count]
    bit = lax.axis_index("group") % 2
    place = jnp.concatenate([place, bit[None].astype(jnp.int32)])

    block = pl.pallas_call(
        pack_kernel,
        out_shape=jax.ShapeDtypeStruct((rows + CODE_ROWS, D), jnp.bfloat16),
        in_specs=vmem(4) + [pl.BlockSpec(memory_space=pltpu.SMEM)],
        out_specs=vmem(1)[0],
        name="pack",
    )(
        features,
        owner_of_image.reshape(1, rows),
        class_slot.reshape(1, rows),
        is_query.reshape(1, rows),
        episode_ways,
    )

    embed = pl.pallas_call(
        embed_kernel,
        out_shape=(
            jax.ShapeDtypeStruct((rows, D), jnp.bfloat16),
            jax.ShapeDtypeStruct((D, rows), jnp.bfloat16),
            jax.ShapeDtypeStruct((CODE_ROWS, rows), jnp.float32),
        ),
        in_specs=vmem(2),
        out_specs=tuple(vmem(3)),
        cost_estimate=pl.CostEstimate(
            flops=2 * rows * D * D, bytes_accessed=4 * D * D, transcendentals=0
        ),
        name="embed",
    )

    blocks = [block]
    fore = back = block
    for k in range(1, count // 2 + 1):
        fore = lax.ppermute(fore, "dp", ahead)
        blocks.append(fore)
        if k <= (count - 1) // 2:
            back = lax.ppermute(back, "dp", behind)
            blocks.append(back)
    parts = [embed(b, head_weight) for b in blocks]

    grad_rows, keep, give, loss = pl.pallas_call(
        functools.partial(main_kernel, count),
        out_shape=(
            jax.ShapeDtypeStruct((rows, D), jnp.bfloat16),
            jax.ShapeDtypeStruct((D // 2, D), jnp.float32),
            jax.ShapeDtypeStruct((D // 2, D), jnp.float32),
            jax.ShapeDtypeStruct((1, 1), jnp.float32),
        ),
        in_specs=[pl.BlockSpec(memory_space=pltpu.SMEM)] + vmem(3 * count + 1),
        out_specs=tuple(vmem(4)),
        scratch_shapes=[
            pltpu.VMEM((total, D), jnp.bfloat16),
            pltpu.VMEM((D, total), jnp.bfloat16),
            pltpu.VMEM((count, CODE_ROWS, rows), jnp.float32),
            pltpu.VMEM((total, D), jnp.bfloat16),
            pltpu.VMEM((classes, total), jnp.float32),
            pltpu.VMEM((classes, total), jnp.bfloat16),
            pltpu.VMEM((classes, total), jnp.bfloat16),
            pltpu.VMEM((classes, total), jnp.bfloat16),
        ],
        name="episodes",
    )(place, *[p[0] for p in parts], *[p[1] for p in parts], *[p[2] for p in parts], head_weight)

    half = keep + lax.ppermute(give, "group", [(i, i ^ 1) for i in range(groups)])
    move = 2
    while move < groups:
        sent = half.astype(jnp.bfloat16)
        other = lax.ppermute(sent, "group", [(i, i ^ move) for i in range(groups)])
        half = sent.astype(jnp.float32) + other.astype(jnp.float32)
        move *= 2
    other = lax.ppermute(half, "group", [(i, i ^ 1) for i in range(groups)])
    low = jnp.where(bit == 0, half, other)
    high = jnp.where(bit == 0, other, half)
    return grad_rows, jnp.concatenate([low, high]), loss.reshape(1)


def solution(mesh):
    in_specs = (
        P(("dp", "group"), None),
        P(),
        P(("dp", "group"), None),
        P(("dp", "group")),
        P(("dp", "group")),
        P(("dp", "group")),
    )
    out_specs = (P(("dp", "group"), None), P(), P(("dp", "group")))

    def on_device(features, head_weight, owner_of_image, class_slot, is_query, episode_ways):
        count, groups = lax.axis_size("dp"), lax.axis_size("group")
        fits = (
            2 <= count <= 8
            and groups > 1
            and groups & (groups - 1) == 0
            and features.shape[0] == 128
            and episode_ways.shape[0] == 1
        )
        run = gathered if fits else routed
        return run(features, head_weight, owner_of_image, class_slot, is_query, episode_ways)

    return jax.shard_map(
        on_device, mesh=mesh, in_specs=in_specs, out_specs=out_specs, check_vma=False
    )
```

```python
import functools

import jax
import jax.numpy as jnp
from jax import lax
from jax.experimental import pallas as pl
from jax.experimental.pallas import tpu as pltpu
from jax.sharding import PartitionSpec as P

D = 512
WAYS_MAX = 50
CODE_ROWS = 8


def episode_losses(embeds, codes, ways_table):
    count_ep = ways_table.shape[0]
    is_live = codes > 0
    code_value = jnp.maximum(codes - 1, 0)
    query_rows = is_live & (code_value % 2 == 1)
    support_rows = is_live & (code_value % 2 == 0)
    slot_value = code_value // 2
    episode = slot_value // WAYS_MAX
    raw_class = slot_value % WAYS_MAX
    episode_hot = episode[:, None] == jnp.arange(count_ep, dtype=jnp.int32)[None, :]
    row_ways = jnp.sum(jnp.where(episode_hot, ways_table[None, :], 0), axis=1)
    label_id = episode * WAYS_MAX + raw_class % row_ways
    classes = jnp.arange(count_ep * WAYS_MAX, dtype=jnp.int32)
    class_hot = label_id[:, None] == classes[None, :]
    support_hot = (class_hot & support_rows[:, None]).astype(jnp.float32)
    counts = jnp.sum(support_hot, axis=0)
    class_sums = jnp.dot(support_hot.T, embeds, precision=lax.Precision.HIGHEST)
    prototypes = class_sums / jnp.maximum(counts, 1.0)[:, None]
    class_ways = jnp.repeat(ways_table, WAYS_MAX)
    class_valid = classes % WAYS_MAX < class_ways
    allowed = (episode[:, None] == (classes // WAYS_MAX)[None, :]) & class_valid[None, :]
    cross_term = jnp.dot(embeds, prototypes.T, precision=lax.Precision.HIGHEST)
    distance = (
        jnp.sum(embeds * embeds, axis=1)[:, None]
        - 2.0 * cross_term
        + jnp.sum(prototypes * prototypes, axis=1)[None, :]
    )
    scores = -distance * D ** (-0.5)
    masked = jnp.where(allowed, scores, -1e30)
    row_max = jnp.max(masked, axis=1, keepdims=True)
    log_total = row_max[:, 0] + jnp.log(jnp.sum(jnp.exp(masked - row_max), axis=1))
    picked = jnp.sum(jnp.where(class_hot, scores, 0.0), axis=1)
    per_query = jnp.where(query_rows, log_total - picked, 0.0)
    hot_float = episode_hot.astype(jnp.float32)
    query_count = jnp.sum(hot_float * query_rows[:, None].astype(jnp.float32), axis=0)
    return jnp.sum(hot_float * per_query[:, None], axis=0) / jnp.maximum(query_count, 1.0)


def times_transpose(left, right):
    return lax.dot_general(
        left, right, (((1,), (1,)), ((), ())), preferred_element_type=jnp.float32
    )


def inner_rows(left, right):
    return lax.dot_general(
        left, right, (((0,), (0,)), ((), ())), preferred_element_type=jnp.float32
    )


def routed(features, head_weight, owner_of_image, class_slot, is_query, episode_ways):
    peers = lax.axis_size("dp")
    row_count = features.shape[0]
    capacity = 2 * row_count // peers
    target = owner_of_image[:, 0]
    one_hot = (target[:, None] == jnp.arange(peers, dtype=jnp.int32)[None, :]).astype(jnp.int32)
    before = jnp.cumsum(one_hot, axis=0) - one_hot
    position = jnp.sum(one_hot * before, axis=1)
    flat_slot = target * capacity + position
    codes = class_slot * 2 + is_query + 1
    send_rows = (
        jnp.zeros((peers * capacity, D), jnp.bfloat16)
        .at[flat_slot]
        .set(features)
        .reshape(peers, capacity, D)
    )
    send_codes = (
        jnp.zeros((peers * capacity,), jnp.int32).at[flat_slot].set(codes).reshape(peers, capacity)
    )
    got_rows, got_codes = (
        lax.all_to_all(send_rows, "dp", split_axis=0, concat_axis=0, tiled=True),
        lax.all_to_all(send_codes, "dp", split_axis=0, concat_axis=0, tiled=True),
    )
    got_rows = got_rows.reshape(peers * capacity, D)
    got_codes = got_codes.reshape(peers * capacity)
    got_embeds = jnp.dot(got_rows, head_weight, preferred_element_type=jnp.float32).astype(
        jnp.bfloat16
    )
    losses, pull = jax.vjp(
        lambda e: episode_losses(e, got_codes, episode_ways), got_embeds.astype(jnp.float32)
    )
    grad_embeds = pull(jnp.ones_like(losses))[0].astype(jnp.bfloat16)
    partial_value = inner_rows(got_rows, grad_embeds)
    outgoing = times_transpose(grad_embeds, head_weight).astype(jnp.bfloat16)
    returned = lax.all_to_all(
        outgoing.reshape(peers, capacity, D), "dp", split_axis=0, concat_axis=0, tiled=True
    )
    own_rows = returned.reshape(peers * capacity, D)[flat_slot]
    grad_weight = lax.psum(partial_value, ("dp", "group"))
    return (own_rows, grad_weight, losses)


def pack_kernel(features, owner, slot, query, ways, block):
    rows = features.shape[0]
    block[:rows, :] = features[...]
    line = lax.broadcasted_iota(jnp.int32, (CODE_ROWS, rows), 0)
    way = jnp.full((1, rows), ways[0], jnp.int32)
    fields = jnp.where(
        line == 0,
        owner[...],
        jnp.where(line == 1, slot[...], jnp.where(line == 2, query[...], way)),
    )
    block[rows:, :] = jnp.zeros((CODE_ROWS, D), jnp.bfloat16)
    block[rows:, :rows] = fields.astype(jnp.float32).astype(jnp.bfloat16)


def split(value):
    high = value.astype(jnp.bfloat16)
    return high, (value - high.astype(jnp.float32)).astype(jnp.bfloat16)


def dot(left, right, on=(1, 0)):
    return lax.dot_general(
        left, right, (((on[0],), (on[1],)), ((), ())), preferred_element_type=jnp.float32
    )


def ring_order(count):
    return [d for d in range(0, count, 2)] + [d for d in range(count - 1, 0, -1) if d % 2]


def ring_steps(count):
    steps = [0]
    for k in range(1, count // 2 + 1):
        steps.append(-k)
        if k <= (count - 1) // 2:
            steps.append(k)
    return steps


def main_kernel(count, *refs):
    blocks, weight = refs[:count], refs[count]
    grad_rows, keep, give, loss = refs[count + 1 : count + 5]
    feats, embeds, lengths, codes, grads, hot_s, g_high, g_low = refs[count + 5 :]
    rows = grad_rows.shape[0]
    total = rows * count
    classes = count * WAYS_MAX
    scale = D ** (-0.5)

    me = lax.axis_index("dp")
    spot = jnp.where(me % 2 == 0, me // 2, count - 1 - me // 2)
    for k, step in enumerate(ring_steps(count)):
        at = lax.rem(spot + (step + count), count)
        device = jnp.where(2 * at < count, 2 * at, 2 * (count - 1 - at) + 1)
        start = pl.multiple_of(device * rows, rows)
        feats[pl.ds(start, rows), :] = blocks[k][:rows, :]
        codes[pl.ds(device, 1)] = blocks[k][rows:, :rows].astype(jnp.float32)[None]

    step = min(total, 256)
    parts = [slice(at, at + step) for at in range(0, total, step)]
    for part in parts:
        values = dot(feats[part, :], weight[...]).astype(jnp.bfloat16)
        embeds[part, :] = values
        wide = values.astype(jnp.float32)
        squares = jnp.sum(wide * wide, axis=1, keepdims=True)
        lengths[:, part] = jnp.broadcast_to(squares, (step, 128)).T[:8, :]

    def field(line):
        return jnp.concatenate([codes[p, line : line + 1, :] for p in range(count)], axis=1)

    owner, slot, query = field(0), field(1), field(2)
    ways = jnp.zeros_like(owner)
    queries = jnp.zeros_like(owner)
    for p in range(count):
        mine = owner == float(p)
        ways = jnp.where(mine, codes[p, 3:4, 0:1], ways)
        total_q = jnp.sum(jnp.where(mine, query, 0.0), axis=1, keepdims=True)
        queries = jnp.where(mine, total_q, queries)
    share = query / jnp.maximum(queries, 1.0)
    label = slot - jnp.floor((slot + 0.5) / ways) * ways
    first = (owner * float(WAYS_MAX)).astype(jnp.int32)
    last = first + ways.astype(jnp.int32)
    own_class = first + label.astype(jnp.int32)
    support_class = jnp.where(query > 0.5, -1, own_class)

    ids = lax.broadcasted_iota(jnp.int32, (classes, total), 0)
    hot_value = jnp.where(ids == support_class, 1.0, 0.0)
    counts = jnp.maximum(jnp.sum(hot_value, axis=1, keepdims=True), 1.0)
    hot_s[...] = hot_value.astype(jnp.bfloat16)
    protos = dot(hot_s[...], embeds[...]) / counts
    p_high, p_low = split(protos)
    p_length = jnp.sum(protos * protos, axis=1, keepdims=True)

    g_sum = jnp.zeros((classes, 1), jnp.float32)
    loss_sum = jnp.zeros((1, 1), jnp.float32)
    row_sums = []
    for part in parts:
        e = embeds[part, :]
        product = dot(p_high, e, (1, 1)) + dot(p_low, e, (1, 1))
        scores = -(lengths[:1, part] - 2.0 * product + p_length) * scale
        c = lax.broadcasted_iota(jnp.int32, (classes, step), 0)
        masked = jnp.where((c >= first[:, part]) & (c < last[:, part]), scores, -1e30)
        top = jnp.max(masked, axis=0, keepdims=True)
        powers = jnp.exp(masked - top)
        norm = jnp.sum(powers, axis=0, keepdims=True)
        is_own = c == own_class[:, part]
        picked = jnp.sum(jnp.where(is_own, scores, 0.0), axis=0, keepdims=True)
        mine = owner[:, part] == me.astype(jnp.float32)
        losses = share[:, part] * (top + jnp.log(norm) - picked)
        loss_sum += jnp.sum(jnp.where(mine, losses, 0.0), axis=1, keepdims=True)
        g = (powers * (1.0 / norm) - jnp.where(is_own, 1.0, 0.0)) * (
            share[:, part] * (2.0 * scale)
        )
        g_sum += jnp.sum(g, axis=1, keepdims=True)
        row_sums.append(jnp.sum(g, axis=0, keepdims=True))
        high, low = split(g)
        g_high[:, part] = high
        g_low[:, part] = low
    loss[...] = loss_sum

    e = embeds[...]
    d_protos = dot(g_high[...], e) + dot(g_low[...], e) - g_sum * protos
    s_high = (d_protos / counts).astype(jnp.bfloat16)
    for part, row_sum in zip(parts, row_sums):
        value = (
            dot(g_high[:, part], p_high, (0, 0))
            + dot(g_low[:, part], p_high, (0, 0))
            + dot(g_high[:, part], p_low, (0, 0))
            + dot(hot_s[:, part], s_high, (0, 0))
        )
        back = jnp.broadcast_to(row_sum, (128, step)).T[:, :1]
        value = value - back * embeds[part, :].astype(jnp.float32)
        grads[part, :] = value.astype(jnp.bfloat16)

    half = D // 2
    bit = lax.axis_index("group") % 2
    keep_at = pl.multiple_of(bit * half, half)
    give_at = pl.multiple_of((1 - bit) * half, half)
    give[...] = dot(feats[:, pl.ds(give_at, half)], grads[...], (0, 0)).astype(give.dtype)
    keep[...] = dot(feats[:, pl.ds(keep_at, half)], grads[...], (0, 0))
    own = grads[pl.ds(pl.multiple_of(me * rows, rows), rows), :]
    grad_rows[...] = dot(own, weight[...], (1, 1)).astype(jnp.bfloat16)


def vmem(n):
    return [pl.BlockSpec(memory_space=pltpu.VMEM)] * n


def gathered(features, head_weight, owner_of_image, class_slot, is_query, episode_ways):
    count = lax.axis_size("dp")
    groups = lax.axis_size("group")
    rows = features.shape[0]
    classes = count * WAYS_MAX
    total = rows * count

    order = ring_order(count)
    ahead = [(order[i], order[(i + 1) % count]) for i in range(count)]
    behind = [(b, a) for a, b in ahead]

    block = pl.pallas_call(
        pack_kernel,
        out_shape=jax.ShapeDtypeStruct((rows + CODE_ROWS, D), jnp.bfloat16),
        in_specs=vmem(4) + [pl.BlockSpec(memory_space=pltpu.SMEM)],
        out_specs=vmem(1)[0],
        compiler_params=pltpu.CompilerParams(vmem_limit_bytes=4 * 2**20),
        name="pack",
    )(
        features,
        owner_of_image.reshape(1, rows),
        class_slot.reshape(1, rows),
        is_query.reshape(1, rows),
        episode_ways,
    )

    blocks = [block]
    fore = back = block
    for k in range(1, count // 2 + 1):
        fore = lax.ppermute(fore, "dp", ahead)
        blocks.append(fore)
        if k <= (count - 1) // 2:
            back = lax.ppermute(back, "dp", behind)
            blocks.append(back)

    grad_rows, keep, give, loss = pl.pallas_call(
        functools.partial(main_kernel, count),
        out_shape=(
            jax.ShapeDtypeStruct((rows, D), jnp.bfloat16),
            jax.ShapeDtypeStruct((D // 2, D), jnp.float32),
            jax.ShapeDtypeStruct((D // 2, D), jnp.bfloat16),
            jax.ShapeDtypeStruct((1, 1), jnp.float32),
        ),
        in_specs=vmem(count + 1),
        out_specs=tuple(vmem(4)),
        scratch_shapes=[
            pltpu.VMEM((total, D), jnp.bfloat16),
            pltpu.VMEM((total, D), jnp.bfloat16),
            pltpu.VMEM((8, total), jnp.float32),
            pltpu.VMEM((count, CODE_ROWS, rows), jnp.float32),
            pltpu.VMEM((total, D), jnp.bfloat16),
            pltpu.VMEM((classes, total), jnp.bfloat16),
            pltpu.VMEM((classes, total), jnp.bfloat16),
            pltpu.VMEM((classes, total), jnp.bfloat16),
        ],
        compiler_params=pltpu.CompilerParams(vmem_limit_bytes=32 * 2**20),
        name="episodes",
    )(*blocks, head_weight)

    half = keep + lax.ppermute(give, "group", [(i, i ^ 1) for i in range(groups)]).astype(
        jnp.float32
    )
    move = 2
    while move < groups:
        sent = half.astype(jnp.bfloat16)
        other = lax.ppermute(sent, "group", [(i, i ^ move) for i in range(groups)])
        half = sent.astype(jnp.float32) + other.astype(jnp.float32)
        move *= 2
    other = lax.ppermute(half, "group", [(i, i ^ 1) for i in range(groups)])
    bit = lax.axis_index("group") % 2
    low = jnp.where(bit == 0, half, other)
    high = jnp.where(bit == 0, other, half)
    return grad_rows, jnp.concatenate([low, high]), loss.reshape(1)


def solution(mesh):
    in_specs = (
        P(("dp", "group"), None),
        P(),
        P(("dp", "group"), None),
        P(("dp", "group")),
        P(("dp", "group")),
        P(("dp", "group")),
    )
    out_specs = (P(("dp", "group"), None), P(), P(("dp", "group")))

    def on_device(features, head_weight, owner_of_image, class_slot, is_query, episode_ways):
        count, groups = lax.axis_size("dp"), lax.axis_size("group")
        fits = (
            2 <= count <= 8
            and groups > 1
            and groups & (groups - 1) == 0
            and features.shape[0] == 128
            and episode_ways.shape[0] == 1
        )
        run = gathered if fits else routed
        return run(features, head_weight, owner_of_image, class_slot, is_query, episode_ways)

    return jax.shard_map(
        on_device, mesh=mesh, in_specs=in_specs, out_specs=out_specs, check_vma=False
    )
```

```python
import functools

import jax
import jax.numpy as jnp
from jax import lax
from jax.experimental import pallas as pl
from jax.experimental.pallas import tpu as pltpu
from jax.sharding import PartitionSpec as P


D = 512
WAYS_MAX = 50
CODE_ROWS = 8


def episode_losses(embeds, codes, ways_table):
    count_ep = ways_table.shape[0]
    is_live = codes > 0
    code_value = jnp.maximum(codes - 1, 0)
    query_rows = is_live & (code_value % 2 == 1)
    support_rows = is_live & (code_value % 2 == 0)
    slot_value = code_value // 2
    episode = slot_value // WAYS_MAX
    raw_class = slot_value % WAYS_MAX
    episode_hot = episode[:, None] == jnp.arange(count_ep, dtype=jnp.int32)[None, :]
    row_ways = jnp.sum(jnp.where(episode_hot, ways_table[None, :], 0), axis=1)
    label_id = episode * WAYS_MAX + raw_class % row_ways
    classes = jnp.arange(count_ep * WAYS_MAX, dtype=jnp.int32)
    class_hot = label_id[:, None] == classes[None, :]
    support_hot = (class_hot & support_rows[:, None]).astype(jnp.float32)
    counts = jnp.sum(support_hot, axis=0)
    class_sums = jnp.dot(support_hot.T, embeds, precision=lax.Precision.HIGHEST)
    prototypes = class_sums / jnp.maximum(counts, 1.0)[:, None]
    class_ways = jnp.repeat(ways_table, WAYS_MAX)
    class_valid = classes % WAYS_MAX < class_ways
    allowed = (episode[:, None] == (classes // WAYS_MAX)[None, :]) & class_valid[None, :]
    cross_term = jnp.dot(embeds, prototypes.T, precision=lax.Precision.HIGHEST)
    distance = (
        jnp.sum(embeds * embeds, axis=1)[:, None]
        - 2.0 * cross_term
        + jnp.sum(prototypes * prototypes, axis=1)[None, :]
    )
    scores = -distance * D ** (-0.5)
    masked = jnp.where(allowed, scores, -1e30)
    row_max = jnp.max(masked, axis=1, keepdims=True)
    log_total = row_max[:, 0] + jnp.log(jnp.sum(jnp.exp(masked - row_max), axis=1))
    picked = jnp.sum(jnp.where(class_hot, scores, 0.0), axis=1)
    per_query = jnp.where(query_rows, log_total - picked, 0.0)
    hot_float = episode_hot.astype(jnp.float32)
    query_count = jnp.sum(hot_float * query_rows[:, None].astype(jnp.float32), axis=0)
    return jnp.sum(hot_float * per_query[:, None], axis=0) / jnp.maximum(query_count, 1.0)


def times_transpose(left, right):
    return lax.dot_general(
        left, right, (((1,), (1,)), ((), ())), preferred_element_type=jnp.float32
    )


def inner_rows(left, right):
    return lax.dot_general(
        left, right, (((0,), (0,)), ((), ())), preferred_element_type=jnp.float32
    )


def routed(features, head_weight, owner_of_image, class_slot, is_query, episode_ways):
    peers = lax.axis_size("dp")
    row_count = features.shape[0]
    capacity = 2 * row_count // peers
    target = owner_of_image[:, 0]
    one_hot = (target[:, None] == jnp.arange(peers, dtype=jnp.int32)[None, :]).astype(jnp.int32)
    before = jnp.cumsum(one_hot, axis=0) - one_hot
    position = jnp.sum(one_hot * before, axis=1)
    flat_slot = target * capacity + position
    codes = class_slot * 2 + is_query + 1
    send_rows = (
        jnp.zeros((peers * capacity, D), jnp.bfloat16)
        .at[flat_slot]
        .set(features)
        .reshape(peers, capacity, D)
    )
    send_codes = (
        jnp.zeros((peers * capacity,), jnp.int32).at[flat_slot].set(codes).reshape(peers, capacity)
    )
    got_rows, got_codes = (
        lax.all_to_all(send_rows, "dp", split_axis=0, concat_axis=0, tiled=True),
        lax.all_to_all(send_codes, "dp", split_axis=0, concat_axis=0, tiled=True),
    )
    got_rows = got_rows.reshape(peers * capacity, D)
    got_codes = got_codes.reshape(peers * capacity)
    got_embeds = jnp.dot(got_rows, head_weight, preferred_element_type=jnp.float32).astype(
        jnp.bfloat16
    )
    losses, pull = jax.vjp(
        lambda e: episode_losses(e, got_codes, episode_ways), got_embeds.astype(jnp.float32)
    )
    grad_embeds = pull(jnp.ones_like(losses))[0].astype(jnp.bfloat16)
    partial_value = inner_rows(got_rows, grad_embeds)
    outgoing = times_transpose(grad_embeds, head_weight).astype(jnp.bfloat16)
    returned = lax.all_to_all(
        outgoing.reshape(peers, capacity, D), "dp", split_axis=0, concat_axis=0, tiled=True
    )
    own_rows = returned.reshape(peers * capacity, D)[flat_slot]
    grad_weight = lax.psum(partial_value, ("dp", "group"))
    return (own_rows, grad_weight, losses)


def pack_kernel(features, owner, slot, query, ways, block, ints, sems):
    rows = features.shape[0]
    copies = [pltpu.make_async_copy(features, block.at[:rows, :], sems.at[0])]
    for k, source in enumerate((owner, slot, query)):
        copies.append(pltpu.make_async_copy(source, ints.at[k], sems.at[k + 1]))
    for copy in copies:
        copy.start()
    block[rows:, :] = jnp.zeros((CODE_ROWS, D), jnp.bfloat16)
    for copy in copies[1:]:
        copy.wait()
    line = lax.broadcasted_iota(jnp.int32, (CODE_ROWS, rows), 0)
    fields = jnp.where(
        line == 0,
        ints[0],
        jnp.where(line == 1, ints[1], jnp.where(line == 2, ints[2], ways[...])),
    )
    block[rows:, :rows] = fields.astype(jnp.float32).astype(jnp.bfloat16)
    copies[0].wait()


def embed_kernel(count, step, block, weight, *refs):
    embeds, turned, codes = refs[-3:]
    rows = block.shape[0] - CODE_ROWS
    device = ring_device(count, step)
    start = pl.multiple_of(device * rows, rows)
    values = dot(block[:rows, :], weight[...]).astype(jnp.bfloat16)
    embeds[pl.ds(start, rows), :] = values
    turned[:, pl.ds(start, rows)] = block[:rows, :].T
    wide = values.astype(jnp.float32)
    squares = jnp.sum(wide * wide, axis=1, keepdims=True)
    lengths = jnp.broadcast_to(squares, (rows, 128)).T[:CODE_ROWS, :rows]
    line = lax.broadcasted_iota(jnp.int32, (CODE_ROWS, rows), 0)
    codes[:, pl.ds(start, rows)] = jnp.where(
        line == 4, lengths, block[rows:, :rows].astype(jnp.float32)
    )


def split(value):
    high = value.astype(jnp.bfloat16)
    return high, (value - high.astype(jnp.float32)).astype(jnp.bfloat16)


def dot(left, right, on=(1, 0)):
    return lax.dot_general(
        left, right, (((on[0],), (on[1],)), ((), ())), preferred_element_type=jnp.float32
    )


def ring_order(count):
    return [d for d in range(0, count, 2)] + [d for d in range(count - 1, 0, -1) if d % 2]


def ring_steps(count):
    steps = [0]
    for k in range(1, count // 2 + 1):
        steps.append(-k)
        if k <= (count - 1) // 2:
            steps.append(k)
    return steps


def ring_device(count, step):
    me = lax.axis_index("dp")
    spot = jnp.where(me % 2 == 0, me // 2, count - 1 - me // 2)
    at = lax.rem(spot + (step + count), count)
    return jnp.where(2 * at < count, 2 * at, 2 * (count - 1 - at) + 1)


def main_kernel(count, embeds, turned, codes, give, grads, loss, hot_s, g_high, g_low):
    total = embeds.shape[0]
    rows = total // count
    classes = count * WAYS_MAX
    scale = D ** (-0.5)
    me = lax.axis_index("dp")
    step = min(total, 256)
    parts = [slice(at, at + step) for at in range(0, total, step)]

    owner, slot, query = codes[0:1, :], codes[1:2, :], codes[2:3, :]
    ways = jnp.zeros_like(owner)
    queries = jnp.zeros_like(owner)
    for p in range(count):
        mine = owner == float(p)
        ways = jnp.where(mine, codes[3:4, p * rows : p * rows + 1], ways)
        total_q = jnp.sum(jnp.where(mine, query, 0.0), axis=1, keepdims=True)
        queries = jnp.where(mine, total_q, queries)
    share = query / jnp.maximum(queries, 1.0)
    label = slot - jnp.floor((slot + 0.5) / ways) * ways
    first = (owner * float(WAYS_MAX)).astype(jnp.int32)
    last = first + ways.astype(jnp.int32)
    own_class = first + label.astype(jnp.int32)
    support_class = jnp.where(query > 0.5, -1, own_class)

    ids = lax.broadcasted_iota(jnp.int32, (classes, total), 0)
    hot_value = jnp.where(ids == support_class, 1.0, 0.0)
    counts = jnp.maximum(jnp.sum(hot_value, axis=1, keepdims=True), 1.0)
    hot_s[...] = hot_value.astype(jnp.bfloat16)
    protos = dot(hot_s[...], embeds[...]) / counts
    p_high, p_low = split(protos)
    p_length = jnp.sum(protos * protos, axis=1, keepdims=True)

    g_sum = jnp.zeros((classes, 1), jnp.float32)
    loss_sum = jnp.zeros((1, 1), jnp.float32)
    row_sums = []
    for part in parts:
        e = embeds[part, :]
        product = dot(p_high, e, (1, 1)) + dot(p_low, e, (1, 1))
        scores = -(codes[4:5, part] - 2.0 * product + p_length) * scale
        c = lax.broadcasted_iota(jnp.int32, (classes, step), 0)
        masked = jnp.where((c >= first[:, part]) & (c < last[:, part]), scores, -1e30)
        top = jnp.max(masked, axis=0, keepdims=True)
        powers = jnp.exp(masked - top)
        norm = jnp.sum(powers, axis=0, keepdims=True)
        is_own = c == own_class[:, part]
        picked = jnp.sum(jnp.where(is_own, scores, 0.0), axis=0, keepdims=True)
        mine = owner[:, part] == me.astype(jnp.float32)
        losses = share[:, part] * (top + jnp.log(norm) - picked)
        loss_sum += jnp.sum(jnp.where(mine, losses, 0.0), axis=1, keepdims=True)
        g = (powers * (1.0 / norm) - jnp.where(is_own, 1.0, 0.0)) * (
            share[:, part] * (2.0 * scale)
        )
        g_sum += jnp.sum(g, axis=1, keepdims=True)
        row_sums.append(jnp.sum(g, axis=0, keepdims=True))
        high, low = split(g)
        g_high[:, part] = high
        g_low[:, part] = low
    loss[...] = jnp.broadcast_to(loss_sum, loss.shape)

    e = embeds[...]
    d_protos = dot(g_high[...], e) + dot(g_low[...], e) - g_sum * protos
    s_high = (d_protos / counts).astype(jnp.bfloat16)
    for part, row_sum in zip(parts, row_sums):
        value = (
            dot(g_high[:, part], p_high, (0, 0))
            + dot(g_low[:, part], p_high, (0, 0))
            + dot(g_high[:, part], p_low, (0, 0))
            + dot(hot_s[:, part], s_high, (0, 0))
        )
        back = jnp.broadcast_to(row_sum, (128, step)).T[:, :1]
        value = value - back * embeds[part, :].astype(jnp.float32)
        grads[part, :] = value.astype(jnp.bfloat16)

    half = D // 2
    other = 1 - lax.axis_index("group") % 2
    give_at = pl.multiple_of(other * half, half)
    give[...] = dot(turned[pl.ds(give_at, half), :], grads[...]).astype(give.dtype)


def rest_kernel(turned, grads, weight, keep, grad_rows):
    rows, half = grad_rows.shape[0], keep.shape[0]
    keep_at = pl.multiple_of(lax.axis_index("group") % 2 * half, half)
    keep[...] = dot(turned[pl.ds(keep_at, half), :], grads[...])
    own = grads[pl.ds(pl.multiple_of(lax.axis_index("dp") * rows, rows), rows), :]
    grad_rows[...] = dot(own, weight[...], (1, 1)).astype(jnp.bfloat16)


def loss_kernel(value, loss):
    loss[...] = value[:1, :1]


def vmem(n):
    return [pl.BlockSpec(memory_space=pltpu.VMEM)] * n


def gathered(features, head_weight, owner_of_image, class_slot, is_query, episode_ways):
    count = lax.axis_size("dp")
    groups = lax.axis_size("group")
    rows = features.shape[0]
    classes = count * WAYS_MAX
    total = rows * count

    order = ring_order(count)
    ahead = [(order[i], order[(i + 1) % count]) for i in range(count)]
    behind = [(b, a) for a, b in ahead]

    hbm = pl.BlockSpec(memory_space=pltpu.HBM)
    block = pl.pallas_call(
        pack_kernel,
        out_shape=jax.ShapeDtypeStruct((rows + CODE_ROWS, D), jnp.bfloat16),
        in_specs=[hbm] * 4 + vmem(1),
        out_specs=vmem(1)[0],
        scratch_shapes=[
            pltpu.VMEM((3, 1, rows), jnp.int32),
            pltpu.SemaphoreType.DMA((4,)),
        ],
        compiler_params=pltpu.CompilerParams(vmem_limit_bytes=4 * 2**20),
        name="pack",
    )(
        *(
            pltpu.with_memory_space_constraint(value, pltpu.HBM)
            for value in (
                features,
                owner_of_image.reshape(1, rows),
                class_slot.reshape(1, rows),
                is_query.reshape(1, rows),
            )
        ),
        episode_ways.reshape(1, 1),
    )

    blocks = [block]
    fore = back = block
    for k in range(1, count // 2 + 1):
        fore = lax.ppermute(fore, "dp", ahead)
        blocks.append(fore)
        if k <= (count - 1) // 2:
            back = lax.ppermute(back, "dp", behind)
            blocks.append(back)

    held = (
        jax.ShapeDtypeStruct((total, D), jnp.bfloat16),
        jax.ShapeDtypeStruct((D, total), jnp.bfloat16),
        jax.ShapeDtypeStruct((CODE_ROWS, total), jnp.float32),
    )
    state = ()
    for step, value in zip(ring_steps(count), blocks):
        state = pl.pallas_call(
            functools.partial(embed_kernel, count, step),
            out_shape=held,
            in_specs=vmem(2 + len(state)),
            out_specs=tuple(vmem(3)),
            input_output_aliases={2 + i: i for i in range(len(state))},
            cost_estimate=pl.CostEstimate(
                flops=16 * 2 * rows * D * D, bytes_accessed=0, transcendentals=0
            ),
            compiler_params=pltpu.CompilerParams(vmem_limit_bytes=8 * 2**20),
            name="embed",
        )(value, head_weight, *state)

    give, grads, loss = pl.pallas_call(
        functools.partial(main_kernel, count),
        out_shape=(
            pltpu.VMEM((D // 2, D), jnp.bfloat16),
            pltpu.VMEM((total, D), jnp.bfloat16),
            pltpu.VMEM((8, 128), jnp.float32),
        ),
        in_specs=vmem(3),
        out_specs=tuple(vmem(3)),
        scratch_shapes=[pltpu.VMEM((classes, total), jnp.bfloat16)] * 3,
        compiler_params=pltpu.CompilerParams(vmem_limit_bytes=32 * 2**20),
        name="episodes",
    )(*state)
    keep, grad_rows = pl.pallas_call(
        rest_kernel,
        out_shape=(
            pltpu.VMEM((D // 2, D), jnp.float32),
            pltpu.VMEM((rows, D), jnp.bfloat16),
        ),
        in_specs=vmem(3),
        out_specs=tuple(vmem(2)),
        cost_estimate=pl.CostEstimate(flops=2**32, bytes_accessed=0, transcendentals=0),
        compiler_params=pltpu.CompilerParams(vmem_limit_bytes=8 * 2**20),
        name="rest",
    )(state[1], grads, head_weight)

    loss = pl.pallas_call(
        loss_kernel,
        out_shape=jax.ShapeDtypeStruct((1, 1), jnp.float32),
        in_specs=vmem(1),
        out_specs=vmem(1)[0],
        cost_estimate=pl.CostEstimate(flops=2**28, bytes_accessed=0, transcendentals=0),
        compiler_params=pltpu.CompilerParams(vmem_limit_bytes=2**20),
        name="loss",
    )(loss)

    pairs = [(i, i ^ 1) for i in range(groups)]
    half = keep + lax.ppermute(give, "group", pairs).astype(jnp.float32)
    terms = [half]
    move = 2
    while move < groups:
        half = sum(terms[1:], terms[0].astype(jnp.float32))
        sent = half.astype(jnp.bfloat16)
        got = lax.ppermute(sent, "group", [(i, i ^ move) for i in range(groups)])
        terms = [sent, got]
        move *= 2
    others = [lax.ppermute(t, "group", pairs) for t in terms]
    half = sum(terms[1:], terms[0].astype(jnp.float32))
    other = sum(others[1:], others[0].astype(jnp.float32))
    bit = lax.axis_index("group") % 2
    low = jnp.where(bit == 0, half, other)
    high = jnp.where(bit == 0, other, half)
    return grad_rows, jnp.concatenate([low, high]), loss.reshape(1)


def solution(mesh):
    in_specs = (
        P(("dp", "group"), None),
        P(),
        P(("dp", "group"), None),
        P(("dp", "group")),
        P(("dp", "group")),
        P(("dp", "group")),
    )
    out_specs = (P(("dp", "group"), None), P(), P(("dp", "group")))

    def on_device(features, head_weight, owner_of_image, class_slot, is_query, episode_ways):
        count, groups = lax.axis_size("dp"), lax.axis_size("group")
        fits = (
            2 <= count <= 8
            and groups > 1
            and groups & (groups - 1) == 0
            and features.shape[0] == 128
            and episode_ways.shape[0] == 1
        )
        run = gathered if fits else routed
        return run(
            features, head_weight, owner_of_image, class_slot, is_query, episode_ways
        )

    return jax.shard_map(
        on_device, mesh=mesh, in_specs=in_specs, out_specs=out_specs, check_vma=False
    )
```

```python
import functools

import jax
import jax.numpy as jnp
from jax import lax
from jax.experimental import pallas as pl
from jax.experimental.pallas import tpu as pltpu
from jax.sharding import PartitionSpec as P


D = 512
WAYS_MAX = 50
CODE_ROWS = 8


def episode_losses(embeds, codes, ways_table):
    count_ep = ways_table.shape[0]
    is_live = codes > 0
    code_value = jnp.maximum(codes - 1, 0)
    query_rows = is_live & (code_value % 2 == 1)
    support_rows = is_live & (code_value % 2 == 0)
    slot_value = code_value // 2
    episode = slot_value // WAYS_MAX
    raw_class = slot_value % WAYS_MAX
    episode_hot = episode[:, None] == jnp.arange(count_ep, dtype=jnp.int32)[None, :]
    row_ways = jnp.sum(jnp.where(episode_hot, ways_table[None, :], 0), axis=1)
    label_id = episode * WAYS_MAX + raw_class % row_ways
    classes = jnp.arange(count_ep * WAYS_MAX, dtype=jnp.int32)
    class_hot = label_id[:, None] == classes[None, :]
    support_hot = (class_hot & support_rows[:, None]).astype(jnp.float32)
    counts = jnp.sum(support_hot, axis=0)
    class_sums = jnp.dot(support_hot.T, embeds, precision=lax.Precision.HIGHEST)
    prototypes = class_sums / jnp.maximum(counts, 1.0)[:, None]
    class_ways = jnp.repeat(ways_table, WAYS_MAX)
    class_valid = classes % WAYS_MAX < class_ways
    allowed = (episode[:, None] == (classes // WAYS_MAX)[None, :]) & class_valid[None, :]
    cross_term = jnp.dot(embeds, prototypes.T, precision=lax.Precision.HIGHEST)
    distance = (
        jnp.sum(embeds * embeds, axis=1)[:, None]
        - 2.0 * cross_term
        + jnp.sum(prototypes * prototypes, axis=1)[None, :]
    )
    scores = -distance * D ** (-0.5)
    masked = jnp.where(allowed, scores, -1e30)
    row_max = jnp.max(masked, axis=1, keepdims=True)
    log_total = row_max[:, 0] + jnp.log(jnp.sum(jnp.exp(masked - row_max), axis=1))
    picked = jnp.sum(jnp.where(class_hot, scores, 0.0), axis=1)
    per_query = jnp.where(query_rows, log_total - picked, 0.0)
    hot_float = episode_hot.astype(jnp.float32)
    query_count = jnp.sum(hot_float * query_rows[:, None].astype(jnp.float32), axis=0)
    return jnp.sum(hot_float * per_query[:, None], axis=0) / jnp.maximum(query_count, 1.0)


def times_transpose(left, right):
    return lax.dot_general(
        left, right, (((1,), (1,)), ((), ())), preferred_element_type=jnp.float32
    )


def inner_rows(left, right):
    return lax.dot_general(
        left, right, (((0,), (0,)), ((), ())), preferred_element_type=jnp.float32
    )


def routed(features, head_weight, owner_of_image, class_slot, is_query, episode_ways):
    peers = lax.axis_size("dp")
    row_count = features.shape[0]
    capacity = 2 * row_count // peers
    target = owner_of_image[:, 0]
    one_hot = (target[:, None] == jnp.arange(peers, dtype=jnp.int32)[None, :]).astype(jnp.int32)
    before = jnp.cumsum(one_hot, axis=0) - one_hot
    position = jnp.sum(one_hot * before, axis=1)
    flat_slot = target * capacity + position
    codes = class_slot * 2 + is_query + 1
    send_rows = (
        jnp.zeros((peers * capacity, D), jnp.bfloat16)
        .at[flat_slot]
        .set(features)
        .reshape(peers, capacity, D)
    )
    send_codes = (
        jnp.zeros((peers * capacity,), jnp.int32).at[flat_slot].set(codes).reshape(peers, capacity)
    )
    got_rows, got_codes = (
        lax.all_to_all(send_rows, "dp", split_axis=0, concat_axis=0, tiled=True),
        lax.all_to_all(send_codes, "dp", split_axis=0, concat_axis=0, tiled=True),
    )
    got_rows = got_rows.reshape(peers * capacity, D)
    got_codes = got_codes.reshape(peers * capacity)
    got_embeds = jnp.dot(got_rows, head_weight, preferred_element_type=jnp.float32).astype(
        jnp.bfloat16
    )
    losses, pull = jax.vjp(
        lambda e: episode_losses(e, got_codes, episode_ways), got_embeds.astype(jnp.float32)
    )
    grad_embeds = pull(jnp.ones_like(losses))[0].astype(jnp.bfloat16)
    partial_value = inner_rows(got_rows, grad_embeds)
    outgoing = times_transpose(grad_embeds, head_weight).astype(jnp.bfloat16)
    returned = lax.all_to_all(
        outgoing.reshape(peers, capacity, D), "dp", split_axis=0, concat_axis=0, tiled=True
    )
    own_rows = returned.reshape(peers * capacity, D)[flat_slot]
    grad_weight = lax.psum(partial_value, ("dp", "group"))
    return (own_rows, grad_weight, losses)


def pack_kernel(features, owner, slot, query, ways, block, ints, sems):
    rows = features.shape[0]
    copies = [pltpu.make_async_copy(features, block.at[:rows, :], sems.at[0])]
    for k, source in enumerate((owner, slot, query)):
        copies.append(pltpu.make_async_copy(source, ints.at[k], sems.at[k + 1]))
    for copy in copies:
        copy.start()
    block[rows:, :] = jnp.zeros((CODE_ROWS, D), jnp.bfloat16)
    for copy in copies[1:]:
        copy.wait()
    line = lax.broadcasted_iota(jnp.int32, (CODE_ROWS, rows), 0)
    fields = jnp.where(
        line == 0,
        ints[0],
        jnp.where(line == 1, ints[1], jnp.where(line == 2, ints[2], ways[...])),
    )
    block[rows:, :rows] = fields.astype(jnp.float32).astype(jnp.bfloat16)
    copies[0].wait()


def embed_kernel(count, step, block, weight, *refs):
    embeds, turned, codes = refs[-3:]
    rows = block.shape[0] - CODE_ROWS
    device = ring_device(count, step)
    start = pl.multiple_of(device * rows, rows)
    values = dot(block[:rows, :], weight[...]).astype(jnp.bfloat16)
    embeds[pl.ds(start, rows), :] = values
    turned[:, pl.ds(start, rows)] = block[:rows, :].T
    wide = values.astype(jnp.float32)
    squares = jnp.sum(wide * wide, axis=1, keepdims=True)
    lengths = jnp.broadcast_to(squares, (rows, 128)).T[:CODE_ROWS, :rows]
    line = lax.broadcasted_iota(jnp.int32, (CODE_ROWS, rows), 0)
    codes[:, pl.ds(start, rows)] = jnp.where(
        line == 4, lengths, block[rows:, :rows].astype(jnp.float32)
    )


def split(value):
    high = value.astype(jnp.bfloat16)
    return high, (value - high.astype(jnp.float32)).astype(jnp.bfloat16)


def dot(left, right, on=(1, 0)):
    return lax.dot_general(
        left, right, (((on[0],), (on[1],)), ((), ())), preferred_element_type=jnp.float32
    )


def ring_order(count):
    return [d for d in range(0, count, 2)] + [d for d in range(count - 1, 0, -1) if d % 2]


def ring_steps(count):
    steps = [0]
    for k in range(1, count // 2 + 1):
        steps.append(-k)
        if k <= (count - 1) // 2:
            steps.append(k)
    return steps


def ring_device(count, step):
    me = lax.axis_index("dp")
    spot = jnp.where(me % 2 == 0, me // 2, count - 1 - me // 2)
    at = lax.rem(spot + (step + count), count)
    return jnp.where(2 * at < count, 2 * at, 2 * (count - 1 - at) + 1)


def main_kernel(count, embeds, turned, codes, give, grads, loss, cross, lefts, rights):
    total = embeds.shape[0]
    rows = total // count
    slots = WAYS_MAX + -WAYS_MAX % 8
    classes = count * slots
    scale = D ** (-0.5)
    me = lax.axis_index("dp")
    step = min(total, 256)
    parts = [slice(at, at + step) for at in range(0, total, step)]
    stretch = [slice(k * classes, (k + 1) * classes) for k in range(4)]

    owner, slot, query = codes[0:1, :], codes[1:2, :], codes[2:3, :]
    members = [owner == float(p) for p in range(count)]
    ways = jnp.zeros_like(owner)
    queries = jnp.zeros_like(owner)
    for p, mine in enumerate(members):
        ways = jnp.where(mine, codes[3:4, p * rows : p * rows + 1], ways)
        total_q = jnp.sum(jnp.where(mine, query, 0.0), axis=1, keepdims=True)
        queries = jnp.where(mine, total_q, queries)
    share = query / jnp.maximum(queries, 1.0)
    label = slot - jnp.floor((slot + 0.5) / ways) * ways
    line = lax.broadcasted_iota(jnp.int32, (16, total), 0).astype(jnp.float32)
    by_owner = jnp.where(line == owner, 1.0, 0.0).astype(jnp.bfloat16)

    def spread(value, *places):
        for p in range(0, count, 2):
            pair = jnp.concatenate([jnp.where(mine, value, 0.0) for mine in members[p : p + 2]])
            pair = pair.astype(jnp.bfloat16)
            for k in places:
                at = k * classes + p * slots
                lefts[at : at + pair.shape[0], :] = pair

    def column(table):
        return jnp.concatenate([table[:, p : p + 1] for p in range(count)])

    ids = lax.broadcasted_iota(jnp.int32, (slots, total), 0).astype(jnp.float32)
    is_own = ids == label
    own_value = jnp.where(is_own, 1.0, 0.0)
    hot_value = jnp.where(query > 0.5, 0.0, own_value)
    spread(hot_value, 3)
    counts = dot(hot_value.astype(jnp.bfloat16), by_owner, (1, 1))
    per_class = column(1.0 / jnp.maximum(counts, 1.0))
    protos = dot(lefts[stretch[3], :], embeds[...]) * per_class
    p_high, p_low = split(protos)
    rights[stretch[0], :] = p_high
    rights[stretch[1], :] = p_high
    rights[stretch[2], :] = p_low
    half_length = 0.5 * jnp.sum(protos * protos, axis=1, keepdims=True)

    for part in parts:
        e = embeds[part, :]
        product = dot(rights[classes : 3 * classes, :], e, (1, 1))
        product = product[:classes, :] + product[classes:, :] - half_length
        picked = jnp.zeros((slots, step), jnp.float32)
        for p, mine in enumerate(members):
            picked = jnp.where(mine[:, part], product[p * slots : (p + 1) * slots, :], picked)
        cross[:, part] = picked
    scores = (2.0 * cross[...] - codes[4:5, :]) * scale
    masked = jnp.where(ids < ways, scores, -1e30)
    top = jnp.max(masked, axis=0, keepdims=True)
    powers = jnp.exp(masked - top)
    norm = jnp.sum(powers, axis=0, keepdims=True)
    picked = jnp.sum(jnp.where(is_own, scores, 0.0), axis=0, keepdims=True)
    losses = share * (top + jnp.log(norm) - picked)
    losses = jnp.where(owner == me.astype(jnp.float32), losses, 0.0)
    loss[...] = jnp.broadcast_to(jnp.sum(losses, axis=1, keepdims=True), loss.shape)
    g = (powers * (1.0 / norm) - own_value) * (share * (2.0 * scale))
    row_sum = jnp.sum(g, axis=0, keepdims=True)
    high, low = split(g)
    spread(high.astype(jnp.float32), 1, 2)
    spread(low.astype(jnp.float32), 0)
    g_sum = column(dot(high, by_owner, (1, 1)) + dot(low, by_owner, (1, 1)))

    e = embeds[...]
    d_protos = dot(lefts[: 2 * classes, :], e)
    d_protos = d_protos[classes:, :] + d_protos[:classes, :] - g_sum * protos
    rights[stretch[3], :] = (d_protos * per_class).astype(jnp.bfloat16)
    wide = min(total, 512)
    for part in [slice(at, at + wide) for at in range(0, total, wide)]:
        value = dot(lefts[:, part], rights[...], (0, 0))
        back = jnp.broadcast_to(row_sum[:, part], (128, wide)).T[:, :1]
        value = value - back * embeds[part, :].astype(jnp.float32)
        grads[part, :] = value.astype(jnp.bfloat16)

    half = D // 2
    other = 1 - lax.axis_index("group") % 2
    give_at = pl.multiple_of(other * half, half)
    give[...] = dot(turned[pl.ds(give_at, half), :], grads[...]).astype(give.dtype)


def rest_kernel(turned, grads, weight, keep, grad_rows):
    rows, half = grad_rows.shape[0], keep.shape[0]
    keep_at = pl.multiple_of(lax.axis_index("group") % 2 * half, half)
    keep[...] = dot(turned[pl.ds(keep_at, half), :], grads[...])
    own = grads[pl.ds(pl.multiple_of(lax.axis_index("dp") * rows, rows), rows), :]
    grad_rows[...] = dot(own, weight[...], (1, 1)).astype(jnp.bfloat16)


def loss_kernel(value, loss):
    loss[...] = value[:1, :1]


def vmem(n):
    return [pl.BlockSpec(memory_space=pltpu.VMEM)] * n


def gathered(features, head_weight, owner_of_image, class_slot, is_query, episode_ways):
    count = lax.axis_size("dp")
    groups = lax.axis_size("group")
    rows = features.shape[0]
    slots = WAYS_MAX + -WAYS_MAX % 8
    total = rows * count

    order = ring_order(count)
    ahead = [(order[i], order[(i + 1) % count]) for i in range(count)]
    behind = [(b, a) for a, b in ahead]

    hbm = pl.BlockSpec(memory_space=pltpu.HBM)
    block = pl.pallas_call(
        pack_kernel,
        out_shape=jax.ShapeDtypeStruct((rows + CODE_ROWS, D), jnp.bfloat16),
        in_specs=[hbm] * 4 + vmem(1),
        out_specs=vmem(1)[0],
        scratch_shapes=[
            pltpu.VMEM((3, 1, rows), jnp.int32),
            pltpu.SemaphoreType.DMA((4,)),
        ],
        compiler_params=pltpu.CompilerParams(vmem_limit_bytes=4 * 2**20),
        name="pack",
    )(
        *(
            pltpu.with_memory_space_constraint(value, pltpu.HBM)
            for value in (
                features,
                owner_of_image.reshape(1, rows),
                class_slot.reshape(1, rows),
                is_query.reshape(1, rows),
            )
        ),
        episode_ways.reshape(1, 1),
    )

    blocks = [block]
    fore = back = block
    for k in range(1, count // 2 + 1):
        fore = lax.ppermute(fore, "dp", ahead)
        blocks.append(fore)
        if k <= (count - 1) // 2:
            back = lax.ppermute(back, "dp", behind)
            blocks.append(back)

    held = (
        jax.ShapeDtypeStruct((total, D), jnp.bfloat16),
        jax.ShapeDtypeStruct((D, total), jnp.bfloat16),
        jax.ShapeDtypeStruct((CODE_ROWS, total), jnp.float32),
    )
    state = ()
    for step, value in zip(ring_steps(count), blocks):
        state = pl.pallas_call(
            functools.partial(embed_kernel, count, step),
            out_shape=held,
            in_specs=vmem(2 + len(state)),
            out_specs=tuple(vmem(3)),
            input_output_aliases={2 + i: i for i in range(len(state))},
            cost_estimate=pl.CostEstimate(
                flops=16 * 2 * rows * D * D, bytes_accessed=0, transcendentals=0
            ),
            compiler_params=pltpu.CompilerParams(vmem_limit_bytes=8 * 2**20),
            name="embed",
        )(value, head_weight, *state)

    give, grads, loss = pl.pallas_call(
        functools.partial(main_kernel, count),
        out_shape=(
            pltpu.VMEM((D // 2, D), jnp.bfloat16),
            pltpu.VMEM((total, D), jnp.bfloat16),
            pltpu.VMEM((8, 128), jnp.float32),
        ),
        in_specs=vmem(3),
        out_specs=tuple(vmem(3)),
        scratch_shapes=[
            pltpu.VMEM((slots, total), jnp.float32),
            pltpu.VMEM((4 * count * slots, total), jnp.bfloat16),
            pltpu.VMEM((4 * count * slots, D), jnp.bfloat16),
        ],
        compiler_params=pltpu.CompilerParams(vmem_limit_bytes=32 * 2**20),
        name="episodes",
    )(*state)
    keep, grad_rows = pl.pallas_call(
        rest_kernel,
        out_shape=(
            pltpu.VMEM((D // 2, D), jnp.float32),
            pltpu.VMEM((rows, D), jnp.bfloat16),
        ),
        in_specs=vmem(3),
        out_specs=tuple(vmem(2)),
        cost_estimate=pl.CostEstimate(flops=2**32, bytes_accessed=0, transcendentals=0),
        compiler_params=pltpu.CompilerParams(vmem_limit_bytes=8 * 2**20),
        name="rest",
    )(state[1], grads, head_weight)

    loss = pl.pallas_call(
        loss_kernel,
        out_shape=jax.ShapeDtypeStruct((1, 1), jnp.float32),
        in_specs=vmem(1),
        out_specs=vmem(1)[0],
        cost_estimate=pl.CostEstimate(flops=2**28, bytes_accessed=0, transcendentals=0),
        compiler_params=pltpu.CompilerParams(vmem_limit_bytes=2**20),
        name="loss",
    )(loss)

    pairs = [(i, i ^ 1) for i in range(groups)]
    half = keep + lax.ppermute(give, "group", pairs).astype(jnp.float32)
    terms = [half]
    move = 2
    while move < groups:
        half = sum(terms[1:], terms[0].astype(jnp.float32))
        sent = half.astype(jnp.bfloat16)
        got = lax.ppermute(sent, "group", [(i, i ^ move) for i in range(groups)])
        terms = [sent, got]
        move *= 2
    others = [lax.ppermute(t, "group", pairs) for t in terms]
    half = sum(terms[1:], terms[0].astype(jnp.float32))
    other = sum(others[1:], others[0].astype(jnp.float32))
    bit = lax.axis_index("group") % 2
    low = jnp.where(bit == 0, half, other)
    high = jnp.where(bit == 0, other, half)
    return grad_rows, jnp.concatenate([low, high]), loss.reshape(1)


def solution(mesh):
    in_specs = (
        P(("dp", "group"), None),
        P(),
        P(("dp", "group"), None),
        P(("dp", "group")),
        P(("dp", "group")),
        P(("dp", "group")),
    )
    out_specs = (P(("dp", "group"), None), P(), P(("dp", "group")))

    def on_device(features, head_weight, owner_of_image, class_slot, is_query, episode_ways):
        count, groups = lax.axis_size("dp"), lax.axis_size("group")
        fits = (
            2 <= count <= 8
            and groups > 1
            and groups & (groups - 1) == 0
            and features.shape[0] == 128
            and episode_ways.shape[0] == 1
        )
        run = gathered if fits else routed
        return run(
            features, head_weight, owner_of_image, class_slot, is_query, episode_ways
        )

    return jax.shard_map(
        on_device, mesh=mesh, in_specs=in_specs, out_specs=out_specs, check_vma=False
    )
```
